32 devices in a mesh: grp: 4 (over z), dev: 8 (over y, x, core).
Axes of the slice: x: 2, y: 2, z: 4, core: 2. Of those that a mesh axis runs over, the one named last changes fastest.
Arguments:
- images: bfloat16 [1536, 1536], P(('grp', 'dev')), may hold values from -1 to 1, as said below
- texts: bfloat16 [1536, 1536], P(('grp', 'dev')), may hold values from -1 to 1, as said below
- logit_scale: float32 [1], replicated, may hold values from 20 to 60
- logit_bias: float32 [1], replicated, may hold values from -12 to -8
Outputs:
- grad_image: float32 [1536, 1536], P(('grp', 'dev'))
- grad_text: float32 [1536, 1536], P(('grp', 'dev'))
- loss: float32 [1], replicated
The draws below stay inside these ranges and needn't reach their ends.
Inputs may be any that keep to these rules, and one draw needn't show every extreme that they name: `images`: every row has length 1 up to bfloat16 rounding. `texts`: every row has length 1 up to bfloat16 rounding.
All inputs are finite; a program needn't handle non-finite values.
Results may differ from the reference program's by a relative error of at most 0.00095.
Values may be sent and summed in bfloat16 or wider, within the bound.
A program may use at most 128 MiB of HBM per device.

```python
import jax
import jax.numpy as jnp
from jax import lax

D = 1536
ROWS = 48
BATCH = 1536
N_DEV = 8


def unit_rows(values):
    return values / jnp.sqrt(jnp.sum(values * values, axis=-1, keepdims=True))


def paired_rows(key):
    spread = 0.65
    column_scale = jnp.exp(spread * jax.random.normal(jax.random.fold_in(key, 11), (D,), jnp.float32))
    image_raw = jax.random.normal(jax.random.fold_in(key, 12), (BATCH, D), jnp.float32)
    noise_raw = jax.random.normal(jax.random.fold_in(key, 13), (BATCH, D), jnp.float32)
    image_dir = unit_rows(image_raw * column_scale[None, :])
    noise_dir = unit_rows(noise_raw * column_scale[None, :])
    text_dir = unit_rows(0.8 * image_dir + 0.6 * noise_dir)
    return (image_dir, text_dir)


def draw_images(key, part):
    return paired_rows(key)[0].astype(jnp.bfloat16)


def draw_texts(key, part):
    return paired_rows(key)[1].astype(jnp.bfloat16)


def setup_inputs(seed: int = 0) -> dict:
    key_list = jax.random.split(jax.random.key(seed), 5)
    return {
        "images": draw_images(jax.random.fold_in(key_list[4], 71), 0),
        "texts": draw_texts(jax.random.fold_in(key_list[4], 71), 0),
        "logit_scale": jnp.clip(jax.random.uniform(key_list[2], (1,), jnp.float32, 20.0, 60.0), 20.0, 60.0),
        "logit_bias": jnp.clip(jax.random.uniform(key_list[3], (1,), jnp.float32, -12.0, -8.0), -12.0, -8.0),
    }


def reference(images, texts, logit_scale, logit_bias):
    logit_mult = logit_scale[0]
    logit_shift = logit_bias[0]
    pair_total = images.shape[0]
    block_rows = N_DEV * ROWS
    block_number = pair_total // block_rows
    text_ids = jnp.arange(pair_total, dtype=jnp.int32)

    def block_step(running, block_index):
        grad_texts, loss_sum = running
        first_row = (block_index * block_rows).astype(jnp.int32)
        left_rows = lax.dynamic_slice_in_dim(images, first_row, block_rows, 0)
        left_ids = first_row + jnp.arange(block_rows, dtype=jnp.int32)
        logits = jnp.dot(left_rows, texts.T, preferred_element_type=jnp.float32) * logit_mult + logit_shift
        matched = left_ids[:, None] == text_ids[None, :]
        labels = jnp.where(matched, 1.0, -1.0).astype(jnp.float32)
        loss_part = -jnp.sum(jax.nn.log_sigmoid(labels * logits))
        weights = (jax.nn.sigmoid(logits) - matched.astype(jnp.float32)).astype(jnp.bfloat16)
        grad_left = logit_mult * jnp.dot(weights, texts, preferred_element_type=jnp.float32)
        grad_texts = grad_texts + logit_mult * jnp.dot(weights.T, left_rows, preferred_element_type=jnp.float32)
        return (grad_texts, loss_sum + loss_part), grad_left

    start_state = (jnp.zeros(texts.shape, jnp.float32), jnp.zeros((), jnp.float32))
    (grad_text, loss_sum), grad_blocks = lax.scan(block_step, start_state, jnp.arange(block_number, dtype=jnp.int32))
    grad_image = grad_blocks.reshape(pair_total, images.shape[1])
    return grad_image, grad_text, (loss_sum / pair_total).reshape(1)
```

```python
import functools
import math

import jax
import jax.numpy as jnp
from jax import lax
from jax.experimental import pallas as pl
from jax.experimental.pallas import tpu as pltpu
from jax.sharding import PartitionSpec as P

MESH = pl.DeviceIdType.MESH
CORES = 2
POWER = 5


def split_chips(members):
    chips = members // CORES
    q_size = math.isqrt(chips)
    while chips % q_size:
        q_size -= 1
    return chips // q_size, q_size


def split_groups(groups):
    sets = math.isqrt(groups)
    while groups % sets:
        sets -= 1
    return sets, groups // sets


def piece_count(rows):
    for pieces in (3, 2):
        if rows % (16 * pieces) == 0:
            return pieces
    return 1


def pair_terms(logits, matched, losses):
    small = jnp.exp(-jnp.abs(logits))
    sigmoid = jnp.where(logits >= 0, 1.0, small) / (1.0 + small)
    weights = sigmoid - matched.astype(jnp.float32)
    if not losses:
        return weights, None
    signed = jnp.where(matched, -logits, logits)
    return weights, jnp.maximum(signed, 0.0) + jnp.log1p(small)


def encode(values, unit):
    scaled = values * unit
    square = scaled * scaled
    return (square * square * scaled).astype(jnp.bfloat16)


def decode(codes, unit):
    codes = codes.astype(jnp.float32)
    size = jnp.exp(jnp.log(jnp.abs(codes)) * (1.0 / POWER)) * (1.0 / unit)
    return jnp.where(codes < 0, -size, size)


def kernel(
    t_sets, i_sets, p_size, q_size, pieces, unit,
    img_hbm, txt_hbm, scale_ref, bias_ref,
    gi_ref, gt_ref, loss_ref,
    img_all, txt_all, acc_i, acc_t, code_i, code_t, part_i, part_t,
    zs_i, zs_t, zr_i, zr_t,
    loss_acc, loss_own, loss_dev, loss_sum, loss_set, loss_all, loss_grp,
    img_recv, img_z, img_plane, img_core,
    txt_recv, txt_z, txt_plane, txt_core,
    pi_send, pi_recv, pt_send, pt_recv,
    zi_send, zi_recv, zt_send, zt_recv,
    ld_send, ld_recv, ls_send, ls_recv, lg_send, lg_recv,
    fetch_sem,
):
    rows, width = img_hbm.shape
    members = p_size * q_size * CORES
    i_count, t_count = t_sets, i_sets
    groups = i_sets * t_sets
    g = lax.axis_index("grp")
    d = lax.axis_index("dev")
    c = lax.rem(d, CORES)
    chip = d // CORES
    q = lax.rem(chip, q_size)
    p = chip // q_size
    a = g // t_sets
    b = lax.rem(g, t_sets)
    home = g // t_count
    step_rows = rows // pieces

    def member(pi, qi, ci):
        return (pi * q_size + qi) * CORES + ci

    def img_group(k):
        return a * i_count + k

    def txt_group(j):
        return b * t_count + j

    t_own = home == b
    t_slot = lax.rem(g, t_count)
    t_place = jnp.where(t_own, t_slot, t_count)
    below, above = home > b, home < b
    t_first = jnp.where(t_own, t_slot, jnp.where(below, t_count - 1, 0))
    t_turn = jnp.where(below, t_count - 1, 1)
    t_order = [lax.rem(t_first + i * t_turn, t_count) for i in range(t_count)]
    i_order = [lax.rem(b + i, i_count) for i in range(i_count)]

    started = []

    def start(make, when=None):
        started.append((make, when))
        if when is None:
            make().start()
        else:
            pl.when(when)(lambda: make().start())

    def remote(src, dst, send, recv, target):
        return pltpu.make_async_remote_copy(
            src_ref=src, dst_ref=dst, send_sem=send, recv_sem=recv, device_id=target, device_id_type=MESH,
        )

    fetches = [
        pltpu.make_async_copy(src, dst, fetch_sem.at[i])
        for i, (src, dst) in enumerate((
            (txt_hbm, txt_all.at[t_place, q, c]), (img_hbm, img_all.at[b, p, c]),
        ))
    ]
    for fetch in fetches:
        fetch.start()
    barrier = pltpu.get_barrier_semaphore()

    def greet(axis, index):
        pl.semaphore_signal(barrier, inc=1, device_id={axis: index}, device_id_type=MESH)

    def txt_target(i):
        return i * t_sets + home

    awaited = (i_count - 1) + (p_size - 1) + (q_size - 1) + 1
    for i in range(1, i_count):
        greet("grp", img_group(i_order[i]))
    for j in range(t_count):
        pl.when(txt_group(j) != g)(functools.partial(lambda j: greet("grp", txt_group(j)), j))
    for i in range(i_sets):
        awaited = awaited + (txt_target(i) != g).astype(jnp.int32)
    for k in range(1, p_size):
        greet("dev", member(lax.rem(p + k, p_size), q, c))
    for k in range(1, q_size):
        greet("dev", member(p, lax.rem(q + k, q_size), c))
    greet("dev", member(p, q, 1 - c))
    pl.semaphore_wait(barrier, awaited)

    class Side:
        def __init__(self, all_ref, recv, zs, ps, cs, me, size, partner):
            self.all, self.recv = all_ref, recv
            self.zs, self.ps, self.cs = zs, ps, cs
            self.me, self.size, self.partner = me, size, partner

        def piece(self, n, m, cc, h):
            return self.all.at[n, m, cc, pl.ds(h * step_rows, step_rows)]

        def arrived(self, n, m, cc, h):
            ref = self.piece(n, m, cc, h)
            remote(ref, ref, self.cs.at[0, 0, 0], self.recv.at[n, m, cc, h], {"dev": member(p, q, 1 - c)}).wait_recv()

        def out(self, n, m, h, send, target, source=None):
            ref = self.piece(n, m, c, h)
            src = ref if source is None else self.piece(source, m, c, h)
            return remote(src, ref, send, self.recv.at[n, m, c, h], target)

        def spread(self, n, h, when=None):
            for k in range(1, self.size):
                other = lax.rem(self.me + k, self.size)
                start(lambda k=k, other=other: self.out(n, self.me, h, self.ps.at[n, k - 1, h], {"dev": self.partner(other)}), when)
            self.pass_on(n, self.me, h, when)

        def pass_on(self, n, m, h, when=None):
            start(lambda: self.out(n, m, h, self.cs.at[n, m, h], {"dev": member(p, q, 1 - c)}), when)

        def relay(self, n, h, own=None):
            if own is None:
                self.arrived(n, self.me, c, h)
            else:
                pl.when(jnp.logical_not(own))(lambda: self.arrived(n, self.me, c, h))
            self.spread(n, h)

        def relay_plane(self, n, h):
            for k in range(1, self.size):
                other = lax.rem(self.me + k, self.size)
                self.arrived(n, other, c, h)
                self.pass_on(n, other, h)

        def complete(self, n):
            for m in range(self.size):
                for h in range(pieces):
                    self.arrived(n, m, 1 - c, h)

    texts = Side(txt_all, txt_recv, txt_z, txt_plane, txt_core, q, q_size, lambda o: member(p, o, c))
    images = Side(img_all, img_recv, img_z, img_plane, img_core, p, p_size, lambda o: member(o, q, c))

    fetches[0].wait()
    for h in range(pieces):
        for i in range(i_sets):
            start(
                lambda i=i, h=h: texts.out(t_slot, q, h, txt_z.at[i, h], {"grp": txt_target(i)}, t_place),
                txt_target(i) != g,
            )
    fetches[1].wait()
    for h in range(pieces):
        for i in range(1, i_count):
            start(lambda i=i, h=h: images.out(b, p, h, img_z.at[i, h], {"grp": img_group(i_order[i])}))
        images.spread(b, h)
    multiplier = scale_ref[0]
    offset = bias_ref[0]

    for h in range(pieces):
        texts.relay(t_order[0], h, t_own)
    for h in range(pieces):
        images.relay_plane(b, h)
    for h in range(pieces):
        for i in range(1, i_count):
            images.relay(i_order[i], h)
        for i in range(1, t_count):
            texts.relay(t_order[i], h)
        texts.relay_plane(t_order[0], h)
    for h in range(pieces):
        for i in range(1, t_count):
            texts.relay_plane(t_order[i], h)
        for i in range(1, i_count):
            images.relay_plane(i_order[i], h)

    def weigh(left, right, row_start, col_start, losses):
        logits = lax.dot_general(left, right, (((1,), (1,)), ((), ())), preferred_element_type=jnp.float32)
        logits = logits * multiplier + offset
        row = lax.broadcasted_iota(jnp.int32, logits.shape, 0) - row_start
        col = lax.broadcasted_iota(jnp.int32, logits.shape, 1) - col_start
        matched = (row == col) & (row >= 0) & (row < rows)
        weights, terms = pair_terms(logits, matched, losses)
        return jnp.dot(weights.astype(jnp.bfloat16), right, preferred_element_type=jnp.float32), terms

    far = 1 << 24

    def image_pass(k, first):
        left = img_all[k, :, c].reshape(p_size * rows, width)
        right = txt_all[0:t_count].reshape(t_count * q_size * CORES * rows, width)
        j = img_group(k) - b * t_count
        col = jnp.where((j >= 0) & (j < t_count), ((j * q_size + q) * CORES + c) * rows, far)
        product, terms = weigh(left, right, p * rows, col, True)
        loss_acc[...] = terms if first else loss_acc[...] + terms
        acc_i[k] = product.reshape(p_size, rows, width)

    def text_pass(j):
        left = txt_all[j, :, c].reshape(q_size * rows, width)
        right = img_all[...].reshape(i_count * p_size * CORES * rows, width)
        k = txt_group(j) - a * i_count
        col = jnp.where((k >= 0) & (k < i_count), ((k * p_size + p) * CORES + c) * rows, far)
        product, _ = weigh(left, right, q * rows, col, False)
        acc_t[j] = product.reshape(q_size, rows, width)

    def part(acc, code, recv_buf, send, recv, side, n, k, h):
        other = lax.rem(side.me + k, side.size)
        window = pl.ds(h * step_rows, step_rows)
        return remote(
            code.at[n, k - 1, window], recv_buf.at[n, side.me, window], send.at[n, k - 1, h], recv.at[n, side.me, h],
            {"dev": side.partner(other)},
        )

    def send_parts(acc, code, recv_buf, send, recv, side, n):
        for h in range(pieces):
            window = pl.ds(h * step_rows, step_rows)
            for k in range(1, side.size):
                other = lax.rem(side.me + k, side.size)
                code[n, k - 1, window] = encode(acc[n, other, window], unit)
                start(lambda k=k, h=h: part(acc, code, recv_buf, send, recv, side, n, k, h))

    def sum_parts(acc, code, recv_buf, send, recv, side, n, h):
        window = pl.ds(h * step_rows, step_rows)
        total = acc[n, side.me, window]
        for k in range(1, side.size):
            other = lax.rem(side.me + k, side.size)
            ref = recv_buf.at[n, other, window]
            remote(ref, ref, send.at[0, 0, 0], recv.at[n, other, h], {"dev": side.partner(other)}).wait_recv()
            total = total + decode(recv_buf[n, other, window], unit)
        return total

    image_parts = (acc_i, code_i, part_i, pi_send, pi_recv, images)
    text_parts = (acc_t, code_t, part_t, pt_send, pt_recv, texts)

    def loss_copy(own, gathered, send, recv, target, me, size, k, slot):
        return remote(own, gathered.at[slot], send.at[k - 1], recv.at[slot], target(lax.rem(me + k, size)))

    def loss_out(value, own, gathered, send, recv, target, me, size):
        own[...] = value
        gathered[me] = value
        for k in range(1, size):
            start(lambda k=k: loss_copy(own, gathered, send, recv, target, me, size, k, me))

    def loss_in(own, gathered, send, recv, target, me, size):
        for k in range(1, size):
            loss_copy(own, gathered, send, recv, target, me, size, k, lax.rem(me + k, size)).wait_recv()
        total = gathered[0]
        for k in range(1, size):
            total = total + gathered[k]
        return total

    over_dev = (loss_own, loss_dev, ld_send, ld_recv, lambda o: {"dev": o}, d, members)
    over_set = (loss_sum, loss_set, ls_send, ls_recv, lambda o: {"grp": a * t_sets + o}, b, t_sets)
    over_sets = (loss_all, loss_grp, lg_send, lg_recv, lambda o: {"grp": o * t_sets + b}, a, i_sets)

    for j in range(t_count):
        texts.complete(j)
    image_pass(b, True)
    send_parts(*image_parts, b)
    for k in range(i_count):
        images.complete(k)
    for i in reversed(range(t_count)):
        text_pass(t_order[i])
        send_parts(*text_parts, t_order[i])
    for i in range(1, i_count):
        image_pass(i_order[i], False)
        send_parts(*image_parts, i_order[i])
    loss_out(jnp.full((8, 128), jnp.sum(loss_acc[...]), jnp.float32), *over_dev)

    def home_text(j, h):
        window = pl.ds(h * step_rows, step_rows)
        return remote(zs_t.at[j, window], zr_t.at[a, window], zt_send.at[j, h], zt_recv.at[a, h], {"grp": txt_group(j)})

    def home_image(k, h):
        window = pl.ds(h * step_rows, step_rows)
        return remote(zs_i.at[k, window], zr_i.at[b, window], zi_send.at[k, h], zi_recv.at[b, h], {"grp": img_group(k)})

    def reduce_text(i, h):
        window = pl.ds(h * step_rows, step_rows)
        j = t_order[i]
        total = sum_parts(*text_parts, j, h)
        if i:
            zs_t[j, window] = encode(total, unit)
            start(lambda: home_text(j, h))
            return

        @pl.when(t_own)
        def _():
            gt_ref[window] = total

        @pl.when(jnp.logical_not(t_own))
        def _():
            zs_t[j, window] = encode(total, unit)
            gt_ref[window] = jnp.zeros((step_rows, width), jnp.float32)

        start(lambda: home_text(j, h), jnp.logical_not(t_own))

    def reduce_image(k, h):
        window = pl.ds(h * step_rows, step_rows)
        zs_i[k, window] = encode(sum_parts(*image_parts, k, h), unit)
        start(lambda: home_image(k, h))

    for h in range(pieces):
        gi_ref[pl.ds(h * step_rows, step_rows)] = sum_parts(*image_parts, b, h)
    for i in reversed(range(1, t_count)):
        for h in range(pieces):
            reduce_text(i, h)
    loss_out(loss_in(*over_dev), *over_set)
    for i in range(1, i_count):
        for h in range(pieces):
            reduce_image(i_order[i], h)
    for h in range(pieces):
        reduce_text(0, h)
    loss_out(loss_in(*over_set), *over_sets)

    def land(ref, buf, sem, n, h):
        window = pl.ds(h * step_rows, step_rows)
        src = buf.at[n, window]
        remote(src, src, zi_send.at[0, 0], sem.at[n, h], {"dev": member(p, q, 1 - c)}).wait_recv()
        ref[window] = ref[window] + decode(buf[n, window], unit)

    for h in range(pieces):
        window = pl.ds(h * step_rows, step_rows)
        for i in range(1, i_count):
            land(gi_ref, zr_i, zi_recv, i_order[i], h)
        gi_ref[window] = multiplier * gi_ref[window]
    for h in range(pieces):
        window = pl.ds(h * step_rows, step_rows)
        for i in range(i_sets):
            pl.when(txt_target(i) != g)(functools.partial(land, gt_ref, zr_t, zt_recv, i, h))
        gt_ref[window] = multiplier * gt_ref[window]
    loss_ref[...] = loss_in(*over_sets) * (1.0 / (rows * members * groups))
    for make, when in started:
        if when is None:
            make().wait_send()
        else:
            pl.when(when)(lambda make=make: make().wait_send())


def write_out(gi_ref, gt_ref, loss_ref, gi_out, gt_out, loss_out):
    gi_out[...] = gi_ref[...]
    gt_out[...] = gt_ref[...]
    loss_out[0] = jnp.max(loss_ref[...])


def shards(groups, members, images, texts, logit_scale, logit_bias):
    rows, width = images.shape
    p_size, q_size = split_chips(members)
    i_sets, t_sets = split_groups(groups)
    i_count, t_count = t_sets, i_sets
    pieces = piece_count(rows)
    f32, bf16 = jnp.float32, jnp.bfloat16
    dma = pltpu.SemaphoreType.DMA
    unit = 2.0 ** math.floor(math.log2(4.9e7 / (1.05 * rows * members * groups)))

    def side_sems(n, targets, size):
        return [
            dma((n, size, CORES, pieces)),
            dma((targets, pieces)),
            dma((n, max(size - 1, 1), pieces)),
            dma((n, size, pieces)),
        ]

    scratch = [
        ((i_count, p_size, CORES, rows, width), bf16),
        ((t_count + 1, q_size, CORES, rows, width), bf16),
        ((i_count, p_size, rows, width), f32),
        ((t_count, q_size, rows, width), f32),
        ((i_count, max(p_size - 1, 1), rows, width), bf16),
        ((t_count, max(q_size - 1, 1), rows, width), bf16),
        ((i_count, p_size, rows, width), bf16),
        ((t_count, q_size, rows, width), bf16),
        ((i_count, rows, width), bf16),
        ((t_count, rows, width), bf16),
        ((i_count, rows, width), bf16),
        ((i_sets, rows, width), bf16),
        ((p_size * rows, t_count * q_size * CORES * rows), f32),
        ((8, 128), f32),
        ((members, 8, 128), f32),
        ((8, 128), f32),
        ((t_sets, 8, 128), f32),
        ((8, 128), f32),
        ((i_sets, 8, 128), f32),
    ]
    held = sum(math.prod(shape) * jnp.dtype(dtype).itemsize for shape, dtype in scratch)
    vmem, smem = pl.BlockSpec(memory_space=pltpu.VMEM), pl.BlockSpec(memory_space=pltpu.SMEM)
    grad_image, grad_text, loss = pl.pallas_call(
        functools.partial(kernel, t_sets, i_sets, p_size, q_size, pieces, unit),
        out_shape=(
            jax.ShapeDtypeStruct((rows, width), f32),
            jax.ShapeDtypeStruct((rows, width), f32),
            jax.ShapeDtypeStruct((8, 128), f32),
        ),
        in_specs=[pl.BlockSpec(memory_space=pl.ANY)] * 2 + [smem] * 2,
        out_specs=(vmem, vmem, vmem),
        scratch_shapes=[
            *(pltpu.VMEM(shape, dtype) for shape, dtype in scratch),
            *side_sems(i_count, i_count, p_size),
            *side_sems(t_count, i_sets, q_size),
            dma((i_count, max(p_size - 1, 1), pieces)), dma((i_count, p_size, pieces)),
            dma((t_count, max(q_size - 1, 1), pieces)), dma((t_count, q_size, pieces)),
            dma((i_count, pieces)), dma((i_count, pieces)),
            dma((t_count, pieces)), dma((i_sets, pieces)),
            dma((members,)), dma((members,)), dma((t_sets,)), dma((t_sets,)), dma((i_sets,)), dma((i_sets,)),
            dma((2,)),
        ],
        compiler_params=pltpu.CompilerParams(
            collective_id=0, has_side_effects=True, vmem_limit_bytes=min(held + (16 << 20), 60 << 20)
        ),
    )(*(pltpu.with_memory_space_constraint(x, pltpu.HBM) for x in (images, texts)), logit_scale, logit_bias)
    return pl.pallas_call(
        write_out,
        out_shape=(
            jax.ShapeDtypeStruct((rows, width), f32),
            jax.ShapeDtypeStruct((rows, width), f32),
            jax.ShapeDtypeStruct((1,), f32),
        ),
        in_specs=[vmem, vmem, vmem],
        out_specs=(vmem, vmem, smem),
        compiler_params=pltpu.CompilerParams(vmem_limit_bytes=4 << 20),
    )(grad_image, grad_text, loss)


def solution(mesh):
    in_specs = (P(("grp", "dev"), None), P(("grp", "dev"), None), P(), P())
    out_specs = (P(("grp", "dev"), None), P(("grp", "dev"), None), P())
    body = functools.partial(shards, mesh.shape["grp"], mesh.shape["dev"])
    return jax.shard_map(body, mesh=mesh, in_specs=in_specs, out_specs=out_specs, check_vma=False)
```

```python
import functools
import math

import jax
import jax.numpy as jnp
from jax import lax
from jax.experimental import pallas as pl
from jax.experimental.pallas import tpu as pltpu
from jax.sharding import PartitionSpec as P

MESH = pl.DeviceIdType.MESH
CORES = 2
POWER = 5


def split_chips(members):
    chips = members // CORES
    q_size = math.isqrt(chips)
    while chips % q_size:
        q_size -= 1
    return chips // q_size, q_size


def split_groups(groups):
    sets = math.isqrt(groups)
    while groups % sets:
        sets -= 1
    return sets, groups // sets


def piece_count(rows):
    for pieces in (3, 2):
        if rows % (16 * pieces) == 0:
            return pieces
    return 1


def pair_terms(logits, matched, losses):
    small = jnp.exp(-jnp.abs(logits))
    sigmoid = jnp.where(logits >= 0, 1.0, small) / (1.0 + small)
    weights = sigmoid - matched.astype(jnp.float32)
    if not losses:
        return weights, None
    signed = jnp.where(matched, -logits, logits)
    return weights, jnp.maximum(signed, 0.0) + jnp.log1p(small)


def encode(values, unit):
    scaled = values * unit
    square = scaled * scaled
    return (square * square * scaled).astype(jnp.bfloat16)


def decode(codes, unit):
    codes = codes.astype(jnp.float32)
    size = jnp.exp(jnp.log(jnp.abs(codes)) * (1.0 / POWER)) * (1.0 / unit)
    return jnp.where(codes < 0, -size, size)


def kernel(
    t_sets, i_sets, p_size, q_size, pieces, unit,
    img_hbm, txt_hbm, scale_ref, bias_ref,
    gi_ref, gt_ref, loss_ref,
    img_all, txt_all, acc_i, acc_t, code_i, code_t, part_i, part_t,
    zs_i, zs_t, zr_i, zr_t,
    loss_acc, loss_own, loss_dev, loss_sum, loss_set, loss_all, loss_grp,
    img_recv, img_both, img_z, img_plane, img_core,
    txt_recv, txt_both, txt_z, txt_plane, txt_core,
    pi_send, pi_recv, pt_send, pt_recv,
    zi_send, zi_recv, zt_send, zt_recv,
    loss_send, loss_recv,
    fetch_sem,
):
    rows, width = img_hbm.shape
    members = p_size * q_size * CORES
    i_count, t_count = t_sets, i_sets
    groups = i_sets * t_sets
    g = lax.axis_index("grp")
    d = lax.axis_index("dev")
    c = lax.rem(d, CORES)
    chip = d // CORES
    q = lax.rem(chip, q_size)
    p = chip // q_size
    a = g // t_sets
    b = lax.rem(g, t_sets)
    home = g // t_count
    step_rows = rows // pieces

    def member(pi, qi, ci):
        return (pi * q_size + qi) * CORES + ci

    def img_group(k):
        return a * i_count + k

    def txt_group(j):
        return b * t_count + j

    t_own = home == b
    t_slot = lax.rem(g, t_count)
    t_place = jnp.where(t_own, t_slot, t_count)
    below, above = home > b, home < b
    t_first = jnp.where(t_own, t_slot, jnp.where(below, t_count - 1, 0))
    t_turn = jnp.where(below, t_count - 1, 1)
    t_order = [lax.rem(t_first + i * t_turn, t_count) for i in range(t_count)]
    i_order = [lax.rem(b + i, i_count) for i in range(i_count)]

    waits = []

    def remote(src, dst, send, recv, target):
        return pltpu.make_async_remote_copy(
            src_ref=src, dst_ref=dst, send_sem=send, recv_sem=recv, device_id=target, device_id_type=MESH,
        )

    def at_end(make, when=None):
        waits.append((make, when))

    fetches = [
        pltpu.make_async_copy(src, dst, fetch_sem.at[i])
        for i, (src, dst) in enumerate((
            (txt_hbm, txt_all.at[t_place, q, c]), (img_hbm, img_all.at[b, p, c]),
        ))
    ]
    for fetch in fetches:
        fetch.start()
    barrier = pltpu.get_barrier_semaphore()

    def greet(axis, index):
        pl.semaphore_signal(barrier, inc=1, device_id={axis: index}, device_id_type=MESH)

    def txt_target(i):
        return i * t_sets + home

    awaited = (i_count - 1) + (p_size - 1) + (q_size - 1) + 1
    for i in range(1, i_count):
        greet("grp", img_group(i_order[i]))
    for j in range(t_count):
        pl.when(txt_group(j) != g)(functools.partial(lambda j: greet("grp", txt_group(j)), j))
    for i in range(i_sets):
        awaited = awaited + (txt_target(i) != g).astype(jnp.int32)
    for k in range(1, p_size):
        greet("dev", member(lax.rem(p + k, p_size), q, c))
    for k in range(1, q_size):
        greet("dev", member(p, lax.rem(q + k, q_size), c))
    greet("dev", member(p, q, 1 - c))
    pl.semaphore_wait(barrier, awaited)

    def from_core(ref, sem):
        remote(ref, ref, fetch_sem.at[0], sem, {"dev": member(p, q, 1 - c)}).wait_recv()

    def sent(ref, sem):
        remote(ref, ref, sem, fetch_sem.at[0], {"dev": member(p, q, 1 - c)}).wait_send()

    class Side:
        def __init__(self, all_ref, count, recv, both, plane, core, me, size, partner):
            self.all, self.count, self.recv, self.both = all_ref, count, recv, both
            self.plane, self.core = plane, core
            self.me, self.size, self.partner = me, size, partner
            for k in range(1, size):
                at_end(lambda k=k: sent(all_ref.at[pl.ds(0, count), me, c], plane.at[k - 1]))
            at_end(lambda: sent(all_ref.at[pl.ds(0, count), :, c], core.at[0]))

        def piece(self, n, m, cc, h):
            return self.all.at[n, m, cc, pl.ds(h * step_rows, step_rows)]

        def arrived(self, n, m, h):
            from_core(self.piece(n, m, c, h), self.recv.at[n, m, h])

        def out(self, n, m, h, send, target, source=None):
            ref = self.piece(n, m, c, h)
            src = ref if source is None else self.piece(source, m, c, h)
            return remote(src, ref, send, self.recv.at[n, m, h], target)

        def pass_on(self, n, m, h):
            ref = self.piece(n, m, c, h)
            remote(ref, ref, self.core.at[0], self.both.at[n], {"dev": member(p, q, 1 - c)}).start()

        def spread(self, n, h):
            for k in range(1, self.size):
                other = lax.rem(self.me + k, self.size)
                self.out(n, self.me, h, self.plane.at[k - 1], {"dev": self.partner(other)}).start()
            self.pass_on(n, self.me, h)

        def relay(self, n, h, own=None):
            if own is None:
                self.arrived(n, self.me, h)
            else:
                pl.when(jnp.logical_not(own))(lambda: self.arrived(n, self.me, h))
            self.spread(n, h)

        def relay_plane(self, n, h):
            for k in range(1, self.size):
                other = lax.rem(self.me + k, self.size)
                self.arrived(n, other, h)
                self.pass_on(n, other, h)

        def complete(self, n):
            from_core(self.all.at[n, :, 1 - c], self.both.at[n])

    texts = Side(txt_all, t_count, txt_recv, txt_both, txt_plane, txt_core, q, q_size, lambda o: member(p, o, c))
    images = Side(img_all, i_count, img_recv, img_both, img_plane, img_core, p, p_size, lambda o: member(o, q, c))

    fetches[1].wait()
    for h in range(pieces):
        for i in range(1, i_count):
            images.out(b, p, h, img_z.at[i - 1], {"grp": img_group(i_order[i])}).start()
        images.spread(b, h)
    for i in range(1, i_count):
        at_end(lambda i=i: sent(img_all.at[b, p, c], img_z.at[i - 1]))
    fetches[0].wait()
    for i in range(i_sets):
        @pl.when(txt_target(i) != g)
        def _():
            for h in range(pieces):
                texts.out(t_slot, q, h, txt_z.at[i], {"grp": txt_target(i)}, t_place).start()

        at_end(lambda i=i: sent(txt_all.at[t_place, q, c], txt_z.at[i]), txt_target(i) != g)
    multiplier = scale_ref[0]
    offset = bias_ref[0]

    last = pieces - 1
    near, rest = t_order[0], t_order[1:]
    for h in range(pieces):
        texts.relay(near, h, t_own)
        for k in i_order[1:]:
            images.relay(k, h)
    for h in range(pieces):
        images.relay_plane(b, h)
    for h in range(pieces):
        texts.relay_plane(near, h)
        for k in i_order[1:]:
            images.relay_plane(k, h)
        if h < last:
            for j in rest:
                texts.relay(j, h)

    def weigh(left, right, row_start, col_start, losses):
        logits = lax.dot_general(left, right, (((1,), (1,)), ((), ())), preferred_element_type=jnp.float32)
        logits = logits * multiplier + offset
        row = lax.broadcasted_iota(jnp.int32, logits.shape, 0) - row_start
        col = lax.broadcasted_iota(jnp.int32, logits.shape, 1) - col_start
        matched = (row == col) & (row >= 0) & (row < rows)
        weights, terms = pair_terms(logits, matched, losses)
        return jnp.dot(weights.astype(jnp.bfloat16), right, preferred_element_type=jnp.float32), terms

    far = 1 << 24

    def image_pass(j, first):
        left = img_all[:, :, c].reshape(i_count * p_size * rows, width)
        right = txt_all[j].reshape(q_size * CORES * rows, width)
        k = txt_group(j) - a * i_count
        col = jnp.where((k >= 0) & (k < i_count), (q * CORES + c) * rows, far)
        product, terms = weigh(left, right, (k * p_size + p) * rows, col, True)
        loss_acc[...] = terms if first else loss_acc[...] + terms
        product = product.reshape(i_count, p_size, rows, width)
        acc_i[...] = product if first else acc_i[...] + product

    def text_pass(j):
        left = txt_all[j, :, c].reshape(q_size * rows, width)
        right = img_all[...].reshape(i_count * p_size * CORES * rows, width)
        k = txt_group(j) - a * i_count
        col = jnp.where((k >= 0) & (k < i_count), ((k * p_size + p) * CORES + c) * rows, far)
        product, _ = weigh(left, right, q * rows, col, False)
        acc_t[j] = product.reshape(q_size, rows, width)

    def send_parts(acc, code, recv_buf, send, recv, side, n):
        for h in range(pieces):
            window = pl.ds(h * step_rows, step_rows)
            for k in range(1, side.size):
                other = lax.rem(side.me + k, side.size)
                code[n, k - 1, window] = encode(acc[n, other, window], unit)
                remote(
                    code.at[n, k - 1, window], recv_buf.at[n, side.me, window], send.at[k - 1], recv.at[n, k - 1, h],
                    {"dev": side.partner(other)},
                ).start()

    def sum_parts(acc, code, recv_buf, send, recv, side, n, h):
        window = pl.ds(h * step_rows, step_rows)
        total = acc[n, side.me, window]
        for k in range(1, side.size):
            other = lax.rem(side.me + k, side.size)
            from_core(recv_buf.at[n, other, window], recv.at[n, side.size - k - 1, h])
            total = total + decode(recv_buf[n, other, window], unit)
        return total

    image_parts = (acc_i, code_i, part_i, pi_send, pi_recv, images)
    text_parts = (acc_t, code_t, part_t, pt_send, pt_recv, texts)

    for acc, code, recv_buf, send, recv, side in (image_parts, text_parts):
        for k in range(1, side.size):
            at_end(lambda code=code, send=send, k=k: sent(code.at[:, k - 1], send.at[k - 1]))

    def loss_out(value, own, gathered, turn, target, me, size):
        own[...] = value
        gathered[0] = value
        for k in range(1, size):
            remote(own, gathered.at[size - k], loss_send.at[turn], loss_recv.at[turn], target(lax.rem(me + k, size))).start()
        if size > 1:
            at_end(lambda: sent(gathered.at[pl.ds(1, size - 1)], loss_send.at[turn]))

    def loss_in(own, gathered, turn, target, me, size):
        if size > 1:
            from_core(gathered.at[pl.ds(1, size - 1)], loss_recv.at[turn])
        return sum((gathered[k] for k in range(1, size)), gathered[0])

    over_dev = (loss_own, loss_dev, 0, lambda o: {"dev": o}, d, members)
    over_set = (loss_sum, loss_set, 1, lambda o: {"grp": a * t_sets + o}, b, t_sets)
    over_sets = (loss_all, loss_grp, 2, lambda o: {"grp": o * t_sets + b}, a, i_sets)

    for k in range(i_count):
        images.complete(k)
    texts.complete(near)
    for j in rest:
        texts.relay(j, last)
    text_pass(near)
    send_parts(*text_parts, near)
    for h in range(last):
        for j in rest:
            texts.relay_plane(j, h)
    image_pass(near, True)
    for j in rest:
        texts.relay_plane(j, last)
    for j in rest:
        texts.complete(j)
        image_pass(j, False)
    loss_out(jnp.full((8, 128), jnp.sum(loss_acc[...]), jnp.float32), *over_dev)
    for i in (*range(1, i_count), 0):
        send_parts(*image_parts, i_order[i])
    for j in reversed(rest):
        text_pass(j)
        send_parts(*text_parts, j)

    def home_text(j, h):
        window = pl.ds(h * step_rows, step_rows)
        return remote(zs_t.at[j, window], zr_t.at[a, window], zt_send.at[j], zt_recv.at[a, h], {"grp": txt_group(j)})

    def home_image(i, h):
        window = pl.ds(h * step_rows, step_rows)
        k = i_order[i]
        return remote(zs_i.at[k, window], zr_i.at[b, window], zi_send.at[i - 1], zi_recv.at[i - 1, h], {"grp": img_group(k)})

    for i in range(1, i_count):
        at_end(lambda i=i: sent(zs_i.at[i_order[i]], zi_send.at[i - 1]))
    for i in range(t_count):
        at_end(lambda j=t_order[i]: sent(zs_t.at[j], zt_send.at[j]), None if i else jnp.logical_not(t_own))

    def reduce_text(i, h):
        window = pl.ds(h * step_rows, step_rows)
        j = t_order[i]
        total = sum_parts(*text_parts, j, h)
        if i:
            zs_t[j, window] = encode(total, unit)
            home_text(j, h).start()
            return

        @pl.when(t_own)
        def _():
            gt_ref[window] = total

        @pl.when(jnp.logical_not(t_own))
        def _():
            zs_t[j, window] = encode(total, unit)
            gt_ref[window] = jnp.zeros((step_rows, width), jnp.float32)
            home_text(j, h).start()

    def reduce_image(i, h):
        window = pl.ds(h * step_rows, step_rows)
        k = i_order[i]
        zs_i[k, window] = encode(sum_parts(*image_parts, k, h), unit)
        home_image(i, h).start()

    for h in range(pieces):
        reduce_text(0, h)
    loss_out(loss_in(*over_dev), *over_set)
    for h in range(pieces):
        for i in range(1, i_count):
            reduce_image(i, h)
        for i in reversed(range(1, t_count)):
            reduce_text(i, h)
    loss_out(loss_in(*over_set), *over_sets)
    for h in range(pieces):
        gi_ref[pl.ds(h * step_rows, step_rows)] = sum_parts(*image_parts, b, h)

    def land(ref, buf, n, sem, h):
        window = pl.ds(h * step_rows, step_rows)
        from_core(buf.at[n, window], sem)
        ref[window] = ref[window] + decode(buf[n, window], unit)

    for h in range(pieces):
        window = pl.ds(h * step_rows, step_rows)
        for i in range(1, i_count):
            land(gi_ref, zr_i, i_order[i], zi_recv.at[i_count - i - 1, h], h)
        gi_ref[window] = multiplier * gi_ref[window]
        for i in range(i_sets):
            pl.when(txt_target(i) != g)(functools.partial(land, gt_ref, zr_t, i, zt_recv.at[i, h], h))
        gt_ref[window] = multiplier * gt_ref[window]
    loss_ref[...] = loss_in(*over_sets) * (1.0 / (rows * members * groups))
    for make, when in waits:
        if when is None:
            make()
        else:
            pl.when(when)(make)


def write_out(gi_ref, gt_ref, loss_ref, gi_out, gt_out, loss_out):
    gi_out[...] = gi_ref[...]
    gt_out[...] = gt_ref[...]
    loss_out[0] = jnp.max(loss_ref[...])


def shards(groups, members, images, texts, logit_scale, logit_bias):
    rows, width = images.shape
    p_size, q_size = split_chips(members)
    i_sets, t_sets = split_groups(groups)
    i_count, t_count = t_sets, i_sets
    pieces = piece_count(rows)
    f32, bf16 = jnp.float32, jnp.bfloat16
    dma = pltpu.SemaphoreType.DMA
    unit = 2.0 ** math.floor(math.log2(4.9e7 / (1.05 * rows * members * groups)))

    def side_sems(n, targets, size):
        return [dma((n, size, pieces)), dma((n,)), dma((max(targets, 1),)), dma((max(size - 1, 1),)), dma((1,))]

    def part_sems(n, size):
        return [dma((max(size - 1, 1),)), dma((n, max(size - 1, 1), pieces))]

    scratch = [
        ((i_count, p_size, CORES, rows, width), bf16),
        ((t_count + 1, q_size, CORES, rows, width), bf16),
        ((i_count, p_size, rows, width), f32),
        ((t_count, q_size, rows, width), f32),
        ((i_count, max(p_size - 1, 1), rows, width), bf16),
        ((t_count, max(q_size - 1, 1), rows, width), bf16),
        ((i_count, p_size, rows, width), bf16),
        ((t_count, q_size, rows, width), bf16),
        ((i_count, rows, width), bf16),
        ((t_count, rows, width), bf16),
        ((i_count, rows, width), bf16),
        ((i_sets, rows, width), bf16),
        ((i_count * p_size * rows, q_size * CORES * rows), f32),
        ((8, 128), f32),
        ((members, 8, 128), f32),
        ((8, 128), f32),
        ((t_sets, 8, 128), f32),
        ((8, 128), f32),
        ((i_sets, 8, 128), f32),
    ]
    held = sum(math.prod(shape) * jnp.dtype(dtype).itemsize for shape, dtype in scratch)
    vmem, smem = pl.BlockSpec(memory_space=pltpu.VMEM), pl.BlockSpec(memory_space=pltpu.SMEM)
    grad_image, grad_text, loss = pl.pallas_call(
        functools.partial(kernel, t_sets, i_sets, p_size, q_size, pieces, unit),
        out_shape=(
            jax.ShapeDtypeStruct((rows, width), f32),
            jax.ShapeDtypeStruct((rows, width), f32),
            jax.ShapeDtypeStruct((8, 128), f32),
        ),
        in_specs=[pl.BlockSpec(memory_space=pl.ANY)] * 2 + [smem] * 2,
        out_specs=(vmem, vmem, vmem),
        scratch_shapes=[
            *(pltpu.VMEM(shape, dtype) for shape, dtype in scratch),
            *side_sems(i_count, i_count - 1, p_size),
            *side_sems(t_count, i_sets, q_size),
            *part_sems(i_count, p_size),
            *part_sems(t_count, q_size),
            dma((max(i_count - 1, 1),)), dma((max(i_count - 1, 1), pieces)),
            dma((t_count,)), dma((i_sets, pieces)),
            dma((3,)), dma((3,)),
            dma((2,)),
        ],
        compiler_params=pltpu.CompilerParams(
            collective_id=0, has_side_effects=True, vmem_limit_bytes=min(held + (16 << 20), 60 << 20)
        ),
    )(*(pltpu.with_memory_space_constraint(x, pltpu.HBM) for x in (images, texts)), logit_scale, logit_bias)
    return pl.pallas_call(
        write_out,
        out_shape=(
            jax.ShapeDtypeStruct((rows, width), f32),
            jax.ShapeDtypeStruct((rows, width), f32),
            jax.ShapeDtypeStruct((1,), f32),
        ),
        in_specs=[vmem, vmem, vmem],
        out_specs=(vmem, vmem, smem),
        compiler_params=pltpu.CompilerParams(vmem_limit_bytes=4 << 20),
    )(grad_image, grad_text, loss)


def solution(mesh):
    in_specs = (P(("grp", "dev"), None), P(("grp", "dev"), None), P(), P())
    out_specs = (P(("grp", "dev"), None), P(("grp", "dev"), None), P())
    body = functools.partial(shards, mesh.shape["grp"], mesh.shape["dev"])
    return jax.shard_map(body, mesh=mesh, in_specs=in_specs, out_specs=out_specs, check_vma=False)
```
